256 devices in a mesh: ep: 64 (over x, z, core), tp: 4 (over y).
Axes of the slice: x: 4, y: 4, z: 8, core: 2. Of those that a mesh axis runs over, the one named last changes fastest.
Arguments:
- hidden_in: bfloat16 [16384, 3584], P('ep', 'tp'), may hold values from -6 to 6
- moe_gain: bfloat16 [3584], replicated, may hold values from 0.099609375 to 1.8984375
- router_weight: bfloat16 [3584, 256], P('tp'), may hold values from -0.09375 to 0.09375
- expert_ids: int32 [16384, 8], P('ep'), may hold values from 0 to 255, all different within a row; in each aligned block of 256 rows (0 to 255, 256 to 511, ...) at most 16 rows name the same one
- shared_gate: bfloat16 [3584, 1024], P(None, 'tp'), may hold values from -0.09375 to 0.09375
- shared_up: bfloat16 [3584, 1024], P(None, 'tp'), may hold values from -0.09375 to 0.09375
- shared_down: bfloat16 [1024, 3584], P('tp'), may hold values from -0.1875 to 0.1875
- expert_gate: bfloat16 [64, 3584, 1024], P('ep', None, 'tp'), may hold values from -0.09375 to 0.09375
- expert_up: bfloat16 [64, 3584, 1024], P('ep', None, 'tp'), may hold values from -0.09375 to 0.09375
- expert_down: bfloat16 [64, 1024, 3584], P('ep', 'tp'), may hold values from -0.1875 to 0.1875
- attn_gain: bfloat16 [3584], P('tp'), may hold values from 0.099609375 to 1.8984375
- kv_down: bfloat16 [3584, 576], P('tp'), may hold values from -0.09375 to 0.09375
- kv_gain: bfloat16 [512], replicated, may hold values from 0.099609375 to 1.8984375
- doc_lengths: int32 [64, 4], P('ep'), may hold values from 1 to 128, 256 in all within a row
- page_table: int32 [64, 4], P('ep'), may hold values from 0 to 3, each once within a row
Outputs:
- layer_out: bfloat16 [16384, 3584], P('ep', 'tp')
- kv_pages: bfloat16 [64, 4, 64, 576], P('ep', 'tp')
The draws below stay inside these ranges and needn't reach their ends.
Inputs may be any that keep to these rules, and one draw needn't show every extreme that they name: `expert_ids`: each row names 8 different experts. Among the rows of one ep index no expert is named more than 16 times. `doc_lengths`: each row sums to 256. `page_table`: each row holds every number below 4 once.
All inputs are finite; a program needn't handle non-finite values.
Results may differ from the reference program's by a relative error of at most 0.0065.
Values may be sent and summed in bfloat16 or wider, within the bound.
A program may use at most 128 MiB of HBM per device.

```python
import math
import jax
import jax.numpy as jnp
import numpy as np
from jax import lax

D = 3584
HID = 1024
SHARED = 1024
ROUTED = 256
TOP = 8
CAP = 16
KVR = 512
PAGE = 64
NDOC = 4
TOK_DEV = 256
LAT = 576
EXPERTS = 64
TOKENS = 16384
BLK = 4
N_EP = 64


def levels(key, extent, cuts, low, high):
    def one(axis_at, blocks):
        draws = jax.random.uniform(jax.random.fold_in(jax.random.fold_in(key, 6), axis_at), (blocks,), jnp.float32, low / len(cuts), high / len(cuts))
        return jnp.repeat(jnp.exp(draws), extent[axis_at] // blocks).reshape((-1,) + (1,) * (len(extent) - axis_at - 1))

    loudness = one(*cuts[0])
    for cut in cuts[1:]:
        loudness = loudness * one(*cut)
    return loudness


def split_up(amount, total, reach, lean):
    portions = [(1 << 20) // math.isqrt(rank ** lean) + 1 for rank in range(2, amount + 1)]
    surplus, counts = total - reach - (amount - 1), [1] * (amount - 1)
    while surplus > 0:
        free = [i for i in range(amount - 1) if counts[i] < reach]
        mass, left = sum([portions[i] for i in free]), surplus
        for i in free:
            addition = min(reach - counts[i], max(1, left * portions[i] // mass), surplus)
            counts[i] = counts[i] + addition
            surplus = surplus - addition
    return np.array([reach] + counts)


def uneven_parts(own_key, amount, total, most, skew):
    if amount == 2:
        one = jax.random.randint(own_key, (), max(1, total - most), min(most, total - 1) + 1)
        return jnp.stack([one, total - one])
    tallies = jnp.asarray(split_up(amount, total, most, skew), jnp.int32)
    pairs = (amount - 1) // 2
    giver, receiver = tallies[1:1 + 2 * pairs:2], tallies[2:2 + 2 * pairs:2]
    margin = jnp.minimum(giver - 1, most - receiver)
    moved = jax.random.randint(jax.random.fold_in(own_key, 1), (pairs,), 0, 1 << 20) % (margin + 1)
    tallies = tallies.at[1:1 + 2 * pairs:2].set(giver - moved).at[2:2 + 2 * pairs:2].set(receiver + moved)
    return tallies[jax.random.permutation(jax.random.fold_in(own_key, 2), amount)]


def deal_out(stream_key, own, number, rows, number_of, top, most, skew):
    ranking = jax.random.permutation(stream_key, number_of)
    heavy_load, usual = load_shares(number_of, rows * top, most, skew, True), load_shares(number_of, rows * top, most, skew, False)
    places = jnp.arange(number_of)

    def named(sizes, turn):
        used = int((sizes > 0).sum())
        fixed = max(1, used // 4)
        shifted = fixed + (places - fixed + turn * (used - fixed)) % max(1, number_of - fixed)
        return jnp.zeros((number_of,), jnp.int32).at[ranking[jnp.where(places < fixed, places, shifted)]].set(jnp.asarray(sizes, jnp.int32))

    sizes = jnp.where(number % 4 == 0, named(heavy_load, number // 4), named(usual, number - number // 4 - 1))
    mixed = jax.random.permutation(jax.random.fold_in(own, 3), number_of)
    source_of, taker = mixed[0:number_of // 2 * 2:2], mixed[1:number_of // 2 * 2:2]
    slack = jnp.minimum(sizes[source_of] - 1, most - sizes[taker]) // 2
    slack = jnp.where((source_of == ranking[0]) | (taker == ranking[0]) | (sizes[taker] == 0), 0, jnp.maximum(slack, 0))
    shifted = jax.random.randint(jax.random.fold_in(own, 4), (number_of // 2,), 0, 1 << 20) % (slack + 1)
    sizes = sizes.at[source_of].add(-shifted).at[taker].add(shifted)
    labels = jnp.searchsorted(jnp.cumsum(sizes), jnp.arange(rows * top), side="right").astype(jnp.int32)
    grid = labels.reshape(top, rows).T
    grid = grid[jax.random.permutation(jax.random.fold_in(own, 1), rows)]
    turn = jax.random.randint(jax.random.fold_in(own, 2), (rows, 1), 0, top)
    return jnp.take_along_axis(grid, (jnp.arange(top)[None, :] + turn) % top, axis=1)


def load_shares(amount, total, limit, lean, full):
    portions = [(1 << 20) // math.isqrt(grade ** lean) + 1 for grade in range(1, amount + 1)]
    largest = limit if full else min(limit, max(-(-total // amount), total * portions[0] // sum(portions)))
    least = 1 if total - largest >= amount - 1 else 0
    counts, rest = [largest] + [least] * (amount - 1), total - largest - least * (amount - 1)
    while rest > 0:
        free = [i for i in range(1, amount) if counts[i] < largest] or [i for i in range(1, amount) if counts[i] < limit]
        mass, remaining = sum([portions[i] for i in free]), rest
        for i in free:
            more = min(limit - counts[i], max(1, remaining * portions[i] // mass), rest)
            counts[i] = counts[i] + more
            rest = rest - more
    return np.array(counts)


def centred(key, dims, scale, limit, split=(), kind=jnp.bfloat16):
    values = scale * jax.random.normal(key, dims, jnp.float32)
    if split:
        values = values * levels(key, dims, split, -0.22, 0.18)
    return jnp.clip(values, -limit, limit).astype(kind)


def setup_inputs(seed: int = 0) -> dict:
    seeds = jax.random.split(jax.random.key(seed), 16)
    hidden_in = centred(seeds[0], (TOKENS, D), 1.0, 6.0, ((0, 64), (1, 4)))
    moe_gain = jnp.clip(1.0 + 0.18 * jax.random.normal(seeds[1], (D,), jnp.float32), 0.099609375, 1.8984375).astype(jnp.bfloat16)
    router_weight = centred(seeds[2], (D, ROUTED), D ** -0.5, 0.09375, ((0, 4),))
    expert_ids_keys = jax.random.split(jax.random.fold_in(seeds[3], 1), TOKENS // TOK_DEV)
    expert_ids_turns = jax.random.permutation(jax.random.fold_in(seeds[3], 3), TOKENS // TOK_DEV)
    expert_ids = jax.vmap(lambda own, number: deal_out(jax.random.fold_in(seeds[3], 2), own, number, TOK_DEV, ROUTED, TOP, CAP, 2))(expert_ids_keys, expert_ids_turns).reshape((TOKENS, TOP))
    shared_gate = centred(seeds[4], (D, SHARED), D ** -0.5, 0.09375, ((1, 4),))
    shared_up = centred(seeds[5], (D, SHARED), D ** -0.5, 0.09375, ((1, 4),))
    shared_down = centred(seeds[6], (SHARED, D), SHARED ** -0.5, 0.1875, ((0, 4),))
    expert_gate = centred(seeds[7], (EXPERTS, D, HID), D ** -0.5, 0.09375, ((0, 64), (2, 4)))
    expert_up = centred(seeds[8], (EXPERTS, D, HID), D ** -0.5, 0.09375, ((0, 64), (2, 4)))
    expert_down = centred(seeds[9], (EXPERTS, HID, D), HID ** -0.5, 0.1875, ((0, 64), (1, 4)))
    attn_gain = jnp.clip(1.0 + 0.18 * jax.random.normal(seeds[10], (D,), jnp.float32), 0.099609375, 1.8984375).astype(jnp.bfloat16)
    kv_down = centred(seeds[11], (D, LAT), D ** -0.5, 0.09375, ((0, 4),))
    kv_gain = jnp.clip(1.0 + 0.18 * jax.random.normal(seeds[12], (KVR,), jnp.float32), 0.099609375, 1.8984375).astype(jnp.bfloat16)
    doc_lengths = jax.vmap(lambda own: uneven_parts(own, NDOC, TOK_DEV, TOK_DEV // 2, 2))(jax.random.split(seeds[13], N_EP)).reshape((N_EP, NDOC)).astype(jnp.int32)
    page_table = jax.vmap(lambda own: jax.random.permutation(own, BLK))(jax.random.split(seeds[14], N_EP)).reshape((N_EP, BLK)).astype(jnp.int32)
    return {"hidden_in": hidden_in, "moe_gain": moe_gain, "router_weight": router_weight, "expert_ids": expert_ids, "shared_gate": shared_gate, "shared_up": shared_up, "shared_down": shared_down, "expert_gate": expert_gate, "expert_up": expert_up, "expert_down": expert_down, "attn_gain": attn_gain, "kv_down": kv_down, "kv_gain": kv_gain, "doc_lengths": doc_lengths, "page_table": page_table}


EPS = 1e-06
ROUTE_SCALE = 2.5
THETA = 10000.0

def silu(values):
    return values / (1.0 + jnp.exp(-values))

def route_weights(logits, expert_ids):
    scores = 1.0 / (1.0 + jnp.exp(-logits))
    picked = jnp.take_along_axis(scores, expert_ids, axis=1)
    return ROUTE_SCALE * picked / lax.optimization_barrier(jnp.sum(picked, axis=1, keepdims=True))

def slot_table(expert_ids, gate_weights, expert_count, capacity):
    token_count = expert_ids.shape[0]
    columns = jnp.arange(expert_count, dtype=jnp.int32)
    matched = expert_ids[:, :, None] == columns[None, None, :]
    weight_rows = lax.optimization_barrier(jnp.sum(jnp.where(matched, gate_weights[:, :, None], 0.0), axis=1))
    chosen = jnp.any(matched, axis=1).astype(jnp.int32)
    before = (jnp.cumsum(chosen, axis=0) - chosen).astype(jnp.int32)
    target = jnp.where(chosen > 0, columns[None, :] * capacity + before, expert_count * capacity).astype(jnp.int32)
    token_index = jnp.broadcast_to(jnp.arange(token_count, dtype=jnp.int32)[:, None], target.shape)
    slot_token = jnp.full((expert_count * capacity + 1,), token_count, jnp.int32).at[target.reshape(-1)].set(token_index.reshape(-1))
    slot_weight = jnp.zeros((expert_count * capacity + 1,), jnp.float32).at[target.reshape(-1)].set(weight_rows.reshape(-1))
    return (slot_token[:-1], slot_weight[:-1])

def positions_of(lengths, token_count):
    doc_ends = jnp.cumsum(lengths).astype(jnp.int32)
    doc_starts = (doc_ends - lengths).astype(jnp.int32)
    token_index = jnp.arange(token_count, dtype=jnp.int32)
    doc_begin = lax.optimization_barrier(jnp.max(jnp.where(doc_starts[None, :] <= token_index[:, None], doc_starts[None, :], 0), axis=1))
    return (token_index - doc_begin).astype(jnp.float32)

def rotate(rope_part, position):
    half_width = rope_part.shape[1] // 2
    frequency = THETA ** (-jnp.arange(half_width, dtype=jnp.float32) * 2.0 / rope_part.shape[1])
    angles = position[:, None] * frequency[None, :]
    cosine = jnp.cos(angles)
    sine_part = jnp.sin(angles)
    first_half = rope_part[:, :half_width]
    second_half = rope_part[:, half_width:]
    return jnp.concatenate([first_half * cosine - second_half * sine_part, second_half * cosine + first_half * sine_part], axis=1)

def finish(latent, position, kv_gain):
    plain_part = latent[:, :KVR]
    row_scale = lax.rsqrt(lax.optimization_barrier(jnp.mean(plain_part * plain_part, axis=1, keepdims=True)) + EPS)
    normed = plain_part * row_scale * kv_gain.astype(jnp.float32)
    return jnp.concatenate([normed, rotate(latent[:, KVR:], position)], axis=1).astype(jnp.bfloat16)

def reference(hidden_in, moe_gain, router_weight, expert_ids, shared_gate, shared_up, shared_down, expert_gate, expert_up, expert_down, attn_gain, kv_down, kv_gain, doc_lengths, page_table):
    stream = hidden_in.astype(jnp.float32)
    inverse = lax.rsqrt(lax.optimization_barrier(jnp.mean(stream * stream, axis=1, keepdims=True)) + EPS)
    normed = (stream * inverse * moe_gain.astype(jnp.float32)).astype(jnp.bfloat16)
    logits = jnp.dot(normed, router_weight, preferred_element_type=jnp.float32)
    gate_weights = route_weights(logits, expert_ids)
    shared_hidden = (silu(jnp.dot(normed, shared_gate, preferred_element_type=jnp.float32)) * jnp.dot(normed, shared_up, preferred_element_type=jnp.float32)).astype(jnp.bfloat16)
    shared_out = jnp.dot(shared_hidden, shared_down, preferred_element_type=jnp.float32)

    def block_table(block_ids, block_gates):
        return slot_table(block_ids, block_gates, EXPERTS, CAP)
    slot_token, slot_weight = jax.vmap(block_table)(expert_ids.reshape(N_EP, TOK_DEV, TOP), gate_weights.reshape(N_EP, TOK_DEV, TOP))
    offsets = jnp.arange(N_EP, dtype=jnp.int32)[:, None] * TOK_DEV
    global_token = jnp.where(slot_token < TOK_DEV, slot_token + offsets, TOKENS).astype(jnp.int32)
    row_index = global_token.reshape(N_EP, EXPERTS, CAP).transpose(1, 0, 2).reshape(EXPERTS, N_EP * CAP)
    row_weight = slot_weight.reshape(N_EP, EXPERTS, CAP).transpose(1, 0, 2).reshape(EXPERTS, N_EP * CAP)
    padded = jnp.concatenate([normed, jnp.zeros((1, D), jnp.bfloat16)], axis=0)

    def one_expert(expert_index, routed):
        chosen_rows = row_index[expert_index]
        inputs = padded[chosen_rows]
        hidden_rows = (silu(jnp.dot(inputs, expert_gate[expert_index], preferred_element_type=jnp.float32)) * jnp.dot(inputs, expert_up[expert_index], preferred_element_type=jnp.float32)).astype(jnp.bfloat16)
        result = jnp.dot(hidden_rows, expert_down[expert_index], preferred_element_type=jnp.float32)
        return routed.at[chosen_rows].add(result * row_weight[expert_index][:, None])
    routed = lax.fori_loop(0, EXPERTS, one_expert, jnp.zeros((TOKENS + 1, D), jnp.float32))
    layer_out = (stream + shared_out + routed[:TOKENS]).astype(jnp.bfloat16)
    out_values = layer_out.astype(jnp.float32)
    scaled = (out_values * attn_gain.astype(jnp.float32)).astype(jnp.bfloat16)
    row_stat = lax.rsqrt(lax.optimization_barrier(jnp.mean(out_values * out_values, axis=1, keepdims=True)) + EPS)
    latent = jnp.dot(scaled, kv_down, preferred_element_type=jnp.float32) * row_stat

    def block_positions(lengths):
        return positions_of(lengths, TOK_DEV)
    positions = jax.vmap(block_positions)(doc_lengths).reshape(TOKENS)
    cache_rows = finish(latent, positions, kv_gain).reshape(N_EP, BLK, PAGE, LAT)

    def pick_pages(block_cache, block_slots):
        return block_cache[block_slots]
    kv_pages = jax.vmap(pick_pages)(cache_rows, page_table)
    return (layer_out, kv_pages)
```

```python
import jax
import jax.numpy as jnp
from jax import lax
from jax.experimental import pallas as pl
from jax.experimental.pallas import tpu as pltpu
from jax.sharding import PartitionSpec as P

CAP = 16
KVR = 512
NX, NZ, NCORE, TP = 4, 8, 2, 4
PLANE = NX * NCORE
FAR = (2, 5, 6, 3, 4)
NEAR = (0, 1, 7)
NFAR, NNEAR = len(FAR), len(NEAR) * PLANE
HALF = NFAR * PLANE // 2
ORDER = (
    ("a", 2), ("a", 5), ("a", 6), ("a", 3), ("sg2",), ("s0", 2), ("s0", 5), ("sg3",), ("n", 0), ("n", 7),
    ("n", 1), ("s1", 2), ("s0", 6), ("a", 4), ("s1", 5), ("shared",), ("s0", 3), ("s2", 2), ("s2", 5),
    ("x", 0), ("s1", 3), ("s3", 2), ("x", 7), ("x", 1), ("s3", 5), ("s0", 4), ("s2", 3), ("s1", 4),
    ("s4", 5), ("s4", 2), ("s3", 3), ("s2", 4), ("s1", 6), ("s3", 4), ("s4", 3), ("s2", 6), ("s4", 4),
    ("s3", 6), ("f1",), ("s4", 6), ("f2",), ("t",),
)

EPS = 1e-06
ROUTE_SCALE = 2.5
THETA = 10000.0


def silu(values):
    return values / (1.0 + jnp.exp(-values))


def dot(a, b):
    return jnp.dot(a, b, preferred_element_type=jnp.float32)


def positions_of(lengths, tokens):
    doc_ends = jnp.cumsum(lengths)
    doc_starts = doc_ends - lengths
    doc_begin = jnp.max(
        jnp.where(doc_starts[None, :] <= tokens[:, None], doc_starts[None, :], 0), axis=1
    )
    return (tokens - doc_begin).astype(jnp.float32)


def rotate(rope_part, position):
    half_width = rope_part.shape[1] // 2
    frequency = THETA ** (-jnp.arange(half_width, dtype=jnp.float32) * 2.0 / rope_part.shape[1])
    angles = position[:, None] * frequency[None, :]
    cosine = jnp.cos(angles)
    sine_part = jnp.sin(angles)
    first_half = rope_part[:, :half_width]
    second_half = rope_part[:, half_width:]
    return jnp.concatenate(
        [
            first_half * cosine - second_half * sine_part,
            second_half * cosine + first_half * sine_part,
        ],
        axis=1,
    )


def finish(latent, position, kv_gain):
    plain_part = latent[:, :KVR]
    row_scale = lax.rsqrt(jnp.mean(plain_part * plain_part, axis=1, keepdims=True) + EPS)
    normed = plain_part * row_scale * kv_gain.astype(jnp.float32)
    return jnp.concatenate([normed, rotate(latent[:, KVR:], position)], axis=1).astype(jnp.bfloat16)


def turned_dot(a, b):
    return lax.dot_general(a, b, (((0,), (0,)), ((), ())), preferred_element_type=jnp.float32)


def whole_kernel(
    h_ref, ids_ref, gain_ref, router_ref, pages_ref, kv_ref,
    sg_ref, su_ref, sd_ref, eg_ref, eu_ref, ed_ref,
    out_ref, lat_ref,
    x0, xf, xd, sf, sd, p0, pf, pd, q10, q20, q1f, q2f, red, tf, td, acc, xn, hs, gs, rk, wk, pk, lt, lr,
    wg, wu, wd,
    w_sem, a_send, a_recv, g1_send, g1_recv, g2_send, g2_recv, q1_send, q1_recv, q2_send, q2_recv,
    t_send, t_recv, d_send, d_recv, b_send, b_recv, k_send, k_recv, l_send, l_recv,
):
    e = lax.axis_index("ep")
    y = lax.axis_index("tp")
    mx, mz, mc = e // (NZ * NCORE), (e // NCORE) % NZ, e % NCORE
    me = mx * NCORE + mc
    up, down, across = (y + 1) % TP, (y + TP - 1) % TP, (y + 2) % TP
    slots, cap, width = h_ref.shape
    tokens = slots * cap
    f32, bf16 = jnp.float32, jnp.bfloat16

    barrier = pltpu.get_barrier_semaphore()

    def greet(dest):
        pl.semaphore_signal(barrier, inc=1, device_id=dest, device_id_type=pl.DeviceIdType.MESH)

    for k in range(1, TP):
        greet((e, (y + k) % TP))

    def greet_expert(n, carry):
        greet(((e + n) % (NX * NZ * NCORE), y))
        return carry

    lax.fori_loop(1, NX * NZ * NCORE, greet_expert, 0)

    def remote(src, dst, send, recv, dest):
        return pltpu.make_async_remote_copy(
            src_ref=src,
            dst_ref=dst,
            send_sem=send,
            recv_sem=recv,
            device_id=dest,
            device_id_type=pl.DeviceIdType.MESH,
        )

    def ring(src, dst, send, recv, to):
        return remote(src, dst, send, recv, (e, to))

    def gather_one(c, side):
        own = xf.at[c - 1, y]
        return ring(own, own, g1_send.at[c, side], g1_recv.at[c, side], (up, down)[side])

    def gather_two(c, side):
        piece = xf.at[c - 1, (down, up)[side], pl.ds(side * (PLANE // 2), PLANE // 2)]
        return ring(piece, piece, g2_send.at[c, side], g2_recv.at[c, side], (up, down)[side])

    def reduce_one(c, side):
        piece = pf.at[c - 1, across, pl.ds(side * (PLANE // 2), PLANE // 2)]
        return ring(piece, q1f.at[c - 1, side], q1_send.at[c, side], q1_recv.at[c, side], (up, down)[side])

    def reduce_two(c, side):
        piece = pf.at[c - 1, (up, down)[side]]
        return ring(piece, q2f.at[c - 1, side], q2_send.at[c, side], q2_recv.at[c, side], (up, down)[side])

    def shared_gather_one(side):
        return ring(h_ref, x0.at[y], g1_send.at[0, side], g1_recv.at[0, side], (up, down)[side])

    def shared_gather_two(side):
        piece = x0.at[(down, up)[side], pl.ds(side * (slots // 2), slots // 2)]
        return ring(piece, piece, g2_send.at[0, side], g2_recv.at[0, side], (up, down)[side])

    def shared_reduce_one(side):
        piece = p0.at[across, pl.ds(side * (slots // 2), slots // 2)]
        return ring(piece, q10.at[side], q1_send.at[0, side], q1_recv.at[0, side], (up, down)[side])

    def shared_reduce_two(side):
        piece = p0.at[(up, down)[side]]
        return ring(piece, q20.at[side], q2_send.at[0, side], q2_recv.at[0, side], (up, down)[side])

    def picks(k):
        return ring(pk.at[y], pk.at[y], k_send.at[k], k_recv.at[k], (y + k + 1) % TP)

    def latents(k):
        to = (y + k + 1) % TP
        return ring(lt.at[to], lr.at[k], l_send.at[k], l_recv.at[k], to)

    def device(dz, i):
        return ((i // NCORE) * NZ + (mz + dz) % NZ) * NCORE + i % NCORE

    loads = [
        pltpu.make_async_copy(src, dst.at[i], w_sem.at[n])
        for n, (src, dst, i) in enumerate(
            ((sg_ref, wg, 0), (su_ref, wu, 0), (sd_ref, wd, 0), (eg_ref, wg, 1), (eu_ref, wu, 1), (ed_ref, wd, 1))
        )
    ]
    for load in loads:
        load.start()
    x0[y] = h_ref[...]

    groups = rk.shape[0]
    ids = ids_ref[...]
    top = ids.shape[0]
    expert_row = lax.broadcasted_iota(jnp.int32, (groups, tokens), 0)
    chosen = jnp.zeros((groups, tokens), f32)
    for k in range(top):
        chosen = jnp.where(ids[k : k + 1, :] == expert_row, 1.0, chosen)
    earlier = lax.broadcasted_iota(jnp.int32, (tokens, tokens), 0)
    later = lax.broadcasted_iota(jnp.int32, (tokens, tokens), 1)
    before = dot(chosen.astype(bf16), jnp.where(earlier < later, 1.0, 0.0).astype(bf16))
    rk[...] = jnp.where(chosen > 0.0, before, -1.0)
    place = lax.broadcasted_iota(jnp.int32, (cap, tokens), 0).astype(f32)

    def one_hot(s, expert):
        gs[pl.ds(s * cap, cap), :] = jnp.where(rk[pl.ds(expert, 1), :] == place, 1.0, 0.0).astype(bf16)

    def weighted(s, expert):
        gs[pl.ds(s * cap, cap), :] = jnp.where(
            rk[pl.ds(expert, 1), :] == place, wk[pl.ds(expert, 1), :], 0.0
        ).astype(bf16)

    def all_peers(send, skip_self=False):
        def body(n, carry):
            send((me + n) % PLANE)
            return carry

        lax.fori_loop(1 if skip_self else 0, PLANE, body, 0)

    for q, dz in enumerate(FAR):
        for i in range(PLANE):
            one_hot(i, device(dz, i))
        sf[q] = (
            dot(gs[0 : PLANE * cap, :], h_ref[...].reshape(tokens, width))
            .astype(bf16)
            .reshape(PLANE, cap, width)
        )

    pl.semaphore_wait(barrier, NX * NZ * NCORE - 1 + TP - 1)
    for side in range(2):
        shared_gather_one(side).start()

    def far_rows(dz):
        q = FAR.index(dz)

        def straight(i):
            remote(sf.at[q, i], xf.at[q, y, me], a_send, a_recv.at[q], (device(dz, i), y)).start()

        all_peers(straight)

    def norm(count, piece):
        def body(i, carry):
            parts = [piece(i, j).astype(f32) for j in range(TP)]
            energy = sum(jnp.sum(v * v, axis=1, keepdims=True) for v in parts)
            inverse = lax.rsqrt(energy / (width * TP) + EPS)
            at = pl.ds(pl.multiple_of(i * cap, cap), cap)
            for j in range(TP):
                xn[at, j * width : (j + 1) * width] = (
                    parts[j] * inverse * gain_ref[:, j * width : (j + 1) * width]
                ).astype(bf16)
            return carry

        lax.fori_loop(0, count, body, 0)

    def units(rows, w):
        a = xn[0:rows, :]
        hs[0:rows, :] = (silu(dot(a, wg[w])) * dot(a, wu[w])).astype(bf16)

    def down_part(rows, w, j):
        return dot(hs[0:rows, :], wd[w, :, j * width : (j + 1) * width])

    def near_rows(dz):
        k = NEAR.index(dz)
        for i in range(PLANE):
            one_hot(i, device(dz, i))
        for j in range(TP):
            part = dot(gs[0 : PLANE * cap, :], x0[j].reshape(tokens, width)).astype(bf16)
            sd[k * PLANE : (k + 1) * PLANE, j] = part.reshape(PLANE, cap, width)

        def send(i):
            remote(
                sd.at[k * PLANE + i], xd.at[k * PLANE + me], d_send, d_recv.at[k], (device(dz, i), y)
            ).start()

        if dz == 0:
            xd[k * PLANE + me] = sd[k * PLANE + me]
        all_peers(send, dz == 0)

    def shared_part():
        norm(slots, lambda i, j: x0[j, i])
        at = pl.ds(pl.multiple_of(y * width, 128), width)
        logits = dot(xn[0:tokens, at], router_ref[...]).T
        expert = lax.broadcasted_iota(jnp.int32, logits.shape, 0)
        for k in range(top):
            pk[y, k : k + 1, :] = jnp.sum(
                jnp.where(expert == ids_ref[k : k + 1, :], logits, 0.0), axis=0, keepdims=True
            )
        for k in range(TP - 1):
            picks(k).start()
        units(tokens, 0)
        for j in range(TP):
            acc[j] = down_part(tokens, 0, j)

    def near_expert(dz):
        k = NEAR.index(dz)
        most = xd.at[pl.ds(k * PLANE, PLANE - 1 if dz == 0 else PLANE)]
        remote(most, most, d_send, d_recv.at[k], (e, up)).wait_recv()
        norm(PLANE, lambda i, j: xd[k * PLANE + i, j])
        units(PLANE * cap, 1)
        for j in range(TP):
            pd[k * PLANE : (k + 1) * PLANE, j] = (
                down_part(PLANE * cap, 1, j).astype(bf16).reshape(PLANE, cap, width)
            )

        def send_back(i):
            remote(
                pd.at[k * PLANE + i], td.at[k * PLANE + me], b_send, b_recv.at[k], (device(NZ - dz, i), y)
            ).start()

        if dz == 0:
            td[k * PLANE + me] = pd[k * PLANE + me]
        all_peers(send_back, dz == 0)

    def gather_start(c):
        remote(xf.at[c - 1, y], xf.at[c - 1, y], a_send, a_recv.at[c - 1], (e, up)).wait_recv()
        for side in range(2):
            gather_one(c, side).start()

    def gather_on(c):
        for side in range(2):
            gather_one(c, side).wait_recv()
            gather_two(c, side).start()

    def far_expert(c):
        for side in range(2):
            gather_two(c, side).wait_recv()
        norm(PLANE, lambda i, j: xf[c - 1, j, i])
        units(PLANE * cap, 1)
        for j in range(TP):
            pf[c - 1, j] = down_part(PLANE * cap, 1, j).astype(bf16).reshape(PLANE, cap, width)
        for side in range(2):
            reduce_one(c, side).start()

    def reduce_on(c):
        for side in range(2):
            reduce_one(c, side).wait_recv()
            at = pl.ds(side * (PLANE // 2), PLANE // 2)
            to = (up, down)[side]
            pf[c - 1, to, at] = (pf[c - 1, to, at].astype(f32) + q1f[c - 1, side].astype(f32)).astype(bf16)
            reduce_two(c, side).start()

    def far_back(c):
        q, dz = c - 1, FAR[c - 1]
        for side in range(2):
            reduce_two(c, side).wait_recv()
        red[q] = (pf[q, y].astype(f32) + q2f[q, 0].astype(f32) + q2f[q, 1].astype(f32)).astype(bf16)

        def straight(i):
            remote(red.at[q, i], tf.at[q * PLANE + me], t_send, t_recv, (device(NZ - dz, i), y)).start()

        all_peers(straight)

    def shared_on():
        for load in loads:
            load.wait()
        for side in range(2):
            shared_gather_one(side).wait_recv()
            shared_gather_two(side).start()

    def shared_ready():
        for side in range(2):
            shared_gather_two(side).wait_recv()

    def join_near():
        for k in range(TP - 1):
            picks(k).wait()
        scores = 1.0 / (1.0 + jnp.exp(-(pk[0] + pk[1] + pk[2] + pk[3])))
        gates = ROUTE_SCALE * scores / jnp.sum(scores, axis=0, keepdims=True)
        weights = jnp.zeros((groups, tokens), f32)
        for k in range(top):
            weights = jnp.where(ids_ref[k : k + 1, :] == expert_row, gates[k : k + 1, :], weights)
        wk[...] = weights
        for k, dz in enumerate(NEAR):
            for i in range(PLANE):
                weighted(k * PLANE + i, device(dz, i))
            most = td.at[pl.ds(k * PLANE, PLANE - 1 if dz == 0 else PLANE)]
            remote(most, most, b_send, b_recv.at[k], (e, up)).wait_recv()
        for j in range(TP):
            part = acc[j] + turned_dot(gs[0 : NNEAR * cap, :], td[:, j].reshape(NNEAR * cap, width))
            p0[j] = part.astype(bf16).reshape(slots, cap, width)
        for side in range(2):
            shared_reduce_one(side).start()

    def shared_reduce_on():
        for side in range(2):
            shared_reduce_one(side).wait_recv()
            at = pl.ds(side * (slots // 2), slots // 2)
            to = (up, down)[side]
            p0[to, at] = (p0[to, at].astype(f32) + q10[side].astype(f32)).astype(bf16)
            shared_reduce_two(side).start()

    def join_far():
        remote(tf, tf, t_send, t_recv, (e, up)).wait_recv()
        total = h_ref[...].reshape(tokens, width).astype(f32)
        for part in range(2):
            for s in range(HALF):
                slot = part * HALF + s
                weighted(s, device(FAR[slot // PLANE], slot % PLANE))
            total = total + turned_dot(
                gs[0 : HALF * cap, :], tf[part * HALF : (part + 1) * HALF].reshape(HALF * cap, width)
            )
        acc[0] = total

    steps = {
        "a": far_rows,
        "n": near_rows,
        "x": near_expert,
        "s0": lambda dz: gather_start(FAR.index(dz) + 1),
        "s1": lambda dz: gather_on(FAR.index(dz) + 1),
        "s2": lambda dz: far_expert(FAR.index(dz) + 1),
        "s3": lambda dz: reduce_on(FAR.index(dz) + 1),
        "s4": lambda dz: far_back(FAR.index(dz) + 1),
        "sg2": shared_on,
        "sg3": shared_ready,
        "shared": shared_part,
        "f1": join_near,
        "f2": shared_reduce_on,
        "t": join_far,
    }
    for name, *offset in ORDER:
        steps[name](*offset)
    for side in range(2):
        shared_reduce_two(side).wait_recv()
    total = acc[0].reshape(slots, cap, width) + p0[y].astype(f32) + q20[0].astype(f32) + q20[1].astype(f32)
    layer = total.reshape(tokens, width).astype(bf16)
    out_ref[...] = layer

    page = tokens // TP
    token = lax.broadcasted_iota(jnp.int32, (page, tokens), 1)
    inside = lax.broadcasted_iota(jnp.int32, (page, tokens), 0)
    paged = jnp.concatenate(
        [
            dot(jnp.where(token == pages_ref[0, j] * page + inside, 1.0, 0.0).astype(bf16), layer)
            for j in range(TP)
        ],
        axis=0,
    )
    energy = jnp.sum(paged * paged, axis=1, keepdims=True)
    scaled = (paged * gain_ref[:, TP * width :]).astype(bf16)
    latent = lax.dot_general(
        scaled, kv_ref[...], (((1,), (1,)), ((), ())), preferred_element_type=f32
    )
    columns = latent.shape[1]
    spare = (lt.shape[2] - columns) // 2
    coarse = energy.astype(bf16)
    fine = (energy - coarse.astype(f32)).astype(bf16)
    for j in range(TP):
        at = slice(j * page, (j + 1) * page)
        lt[j, :, 0:columns] = latent[at, :].astype(bf16)
        lt[j, :, columns : columns + spare] = jnp.broadcast_to(coarse[at, :], (page, spare))
        lt[j, :, columns + spare :] = jnp.broadcast_to(fine[at, :], (page, spare))
    for k in range(TP - 1):
        latents(k).start()
    for k in range(TP - 1):
        latents(k).wait()
    lat_ref[...] = lt[y].astype(f32) + lr[0].astype(f32) + lr[1].astype(f32) + lr[2].astype(f32)

    for side in range(2):
        shared_gather_one(side).wait_send()
        shared_gather_two(side).wait_send()
        shared_reduce_one(side).wait_send()
        shared_reduce_two(side).wait_send()

    def drain(c, carry):
        for side in range(2):
            gather_one(c, side).wait_send()
            gather_two(c, side).wait_send()
            reduce_one(c, side).wait_send()
            reduce_two(c, side).wait_send()
        return carry

    lax.fori_loop(1, NFAR + 1, drain, 0)
    remote(sf, sf, a_send, t_recv, (e, up)).wait_send()
    remote(red, red, t_send, t_recv, (e, up)).wait_send()
    most = sd.at[pl.ds(0, NNEAR - 1)]
    remote(most, most, d_send, t_recv, (e, up)).wait_send()
    remote(most, most, b_send, t_recv, (e, up)).wait_send()


def whole(hidden, ids, gain, router, pages, kv, weights):
    slots, cap, width = hidden.shape
    tokens = slots * cap
    f32, bf16 = jnp.float32, jnp.bfloat16
    hidden_units = weights[0].shape[1]
    latent = -(-(kv.shape[0] + 1) // 128) * 128
    vmem, hbm = pl.BlockSpec(memory_space=pltpu.VMEM), pl.BlockSpec(memory_space=pl.ANY)
    dma = pltpu.SemaphoreType.DMA
    pair = dma((NFAR + 1, 2))
    block = (slots, cap, width)
    strip = (PLANE, cap, width)
    return pl.pallas_call(
        whole_kernel,
        out_shape=(
            jax.ShapeDtypeStruct((tokens, width), bf16),
            jax.ShapeDtypeStruct((tokens // TP, latent), f32),
        ),
        in_specs=[vmem] * 4 + [pl.BlockSpec(memory_space=pltpu.SMEM), vmem] + [hbm] * 6,
        out_specs=(vmem, vmem),
        scratch_shapes=[
            pltpu.VMEM((TP, *block), bf16),
            pltpu.VMEM((NFAR, TP, *strip), bf16),
            pltpu.VMEM((NNEAR, TP, cap, width), bf16),
            pltpu.VMEM((NFAR, *strip), bf16),
            pltpu.VMEM((NNEAR, TP, cap, width), bf16),
            pltpu.VMEM((TP, *block), bf16),
            pltpu.VMEM((NFAR, TP, *strip), bf16),
            pltpu.VMEM((NNEAR, TP, cap, width), bf16),
            pltpu.VMEM((2, slots // 2, cap, width), bf16),
            pltpu.VMEM((2, *block), bf16),
            pltpu.VMEM((NFAR, 2, PLANE // 2, cap, width), bf16),
            pltpu.VMEM((NFAR, 2, *strip), bf16),
            pltpu.VMEM((NFAR, *strip), bf16),
            pltpu.VMEM((NFAR * PLANE, cap, width), bf16),
            pltpu.VMEM((NNEAR, TP, cap, width), bf16),
            pltpu.VMEM((TP, tokens, width), f32),
            pltpu.VMEM((tokens, width * TP), bf16),
            pltpu.VMEM((tokens, hidden_units), bf16),
            pltpu.VMEM((max(NNEAR, HALF) * cap, tokens), bf16),
            pltpu.VMEM((NX * NZ * NCORE, tokens), f32),
            pltpu.VMEM((NX * NZ * NCORE, tokens), f32),
            pltpu.VMEM((TP, *ids.shape), f32),
            pltpu.VMEM((TP, tokens // TP, latent), bf16),
            pltpu.VMEM((TP - 1, tokens // TP, latent), bf16),
            pltpu.VMEM((2, width * TP, hidden_units), bf16),
            pltpu.VMEM((2, width * TP, hidden_units), bf16),
            pltpu.VMEM((2, hidden_units, width * TP), bf16),
            dma((6,)),
            dma,
            dma((NFAR,)),
            pair, pair, pair, pair, pair, pair, pair, pair,
            dma, dma, dma, dma((len(NEAR),)), dma, dma((len(NEAR),)),
            dma((TP - 1,)), dma((TP - 1,)), dma((TP - 1,)), dma((TP - 1,)),
        ],
        compiler_params=pltpu.CompilerParams(
            collective_id=0, has_side_effects=True, vmem_limit_bytes=67000000
        ),
    )(hidden, ids, gain, router, pages, kv, *weights)


def per_device(
    hidden_in,
    moe_gain,
    router_weight,
    expert_ids,
    shared_gate,
    shared_up,
    shared_down,
    expert_gate,
    expert_up,
    expert_down,
    attn_gain,
    kv_down,
    kv_gain,
    doc_lengths,
    page_table,
):
    tp_count = lax.axis_size("tp")
    member = lax.axis_index("tp")
    tok_rows, width_local = hidden_in.shape
    full_width = width_local * tp_count
    f32 = jnp.float32
    page_count = page_table.shape[1]
    page_len = tok_rows // page_count

    layer_out, sums = whole(
        hidden_in.reshape(tok_rows // CAP, CAP, width_local),
        expert_ids.T,
        jnp.concatenate([moe_gain, attn_gain]).astype(f32).reshape(1, full_width + width_local),
        router_weight,
        page_table,
        kv_down.T,
        (shared_gate, shared_up, shared_down, expert_gate[0], expert_up[0], expert_down[0]),
    )

    slot = jnp.arange(page_count, dtype=jnp.int32)
    own_page = jnp.sum(jnp.where(slot == member, page_table[0], 0))
    tokens = own_page * page_len + jnp.arange(page_len, dtype=jnp.int32)
    columns = kv_down.shape[1]
    latent = sums[:, :columns] * lax.rsqrt(sums[:, columns : columns + 1] / full_width + EPS)
    page_out = finish(latent, positions_of(doc_lengths[0], tokens), kv_gain)
    return (layer_out, page_out.reshape(1, page_count // tp_count, page_len, -1))


def solution(mesh):
    placed = (
        P("ep", "tp"),
        P(),
        P("tp", None),
        P("ep", None),
        P(None, "tp"),
        P(None, "tp"),
        P("tp", None),
        P("ep", None, "tp"),
        P("ep", None, "tp"),
        P("ep", "tp", None),
        P("tp"),
        P("tp", None),
        P(),
        P("ep", None),
        P("ep", None),
    )
    return jax.shard_map(
        per_device,
        mesh=mesh,
        in_specs=placed,
        out_specs=(P("ep", "tp"), P("ep", "tp", None, None)),
        check_vma=False,
    )
```

```python
import jax
import jax.numpy as jnp
from jax import lax
from jax.experimental import pallas as pl
from jax.experimental.pallas import tpu as pltpu
from jax.sharding import PartitionSpec as P

CAP = 16
KVR = 512
NX, NZ, NCORE, TP = 4, 8, 2, 4
PLANE = NX * NCORE
FAR = (2, 7, 3, 5, 4, 6)
NEAR = (0, 1)
NFAR, NNEAR = len(FAR), len(NEAR) * PLANE
HALF = NFAR * PLANE // 2
ORDER = (
    ("a", 2), ("a", 7), ("a", 3), ("a", 5), ("a", 4), ("s0", 7), ("s0", 2), ("sg2",), ("a", 6), ("s1", 2),
    ("s0", 5), ("s0", 3), ("sg3",), ("n", 1), ("s2", 2), ("n", 0), ("s1", 5), ("s0", 4), ("s3", 2),
    ("s2", 5), ("s0", 6), ("shared",), ("s1", 4), ("s4", 2), ("s3", 5), ("s1", 3), ("x", 1), ("s1", 6),
    ("s2", 4), ("s4", 5), ("s1", 7), ("s2", 3), ("s3", 4), ("s2", 6), ("x", 0), ("s3", 3), ("s4", 4),
    ("s3", 6), ("s2", 7), ("f1",), ("s4", 3), ("s4", 6), ("s3", 7), ("f2",), ("s4", 7), ("t",),
)

EPS = 1e-06
ROUTE_SCALE = 2.5
THETA = 10000.0


def silu(values):
    return values / (1.0 + jnp.exp(-values))


def dot(a, b):
    return jnp.dot(a, b, preferred_element_type=jnp.float32)


def positions_of(lengths, tokens):
    doc_ends = jnp.cumsum(lengths)
    doc_starts = doc_ends - lengths
    doc_begin = jnp.max(
        jnp.where(doc_starts[None, :] <= tokens[:, None], doc_starts[None, :], 0), axis=1
    )
    return (tokens - doc_begin).astype(jnp.float32)


def rotate(rope_part, position):
    half_width = rope_part.shape[1] // 2
    frequency = THETA ** (-jnp.arange(half_width, dtype=jnp.float32) * 2.0 / rope_part.shape[1])
    angles = position[:, None] * frequency[None, :]
    cosine = jnp.cos(angles)
    sine_part = jnp.sin(angles)
    first_half = rope_part[:, :half_width]
    second_half = rope_part[:, half_width:]
    return jnp.concatenate(
        [
            first_half * cosine - second_half * sine_part,
            second_half * cosine + first_half * sine_part,
        ],
        axis=1,
    )


def finish(latent, position, kv_gain):
    plain_part = latent[:, :KVR]
    row_scale = lax.rsqrt(jnp.mean(plain_part * plain_part, axis=1, keepdims=True) + EPS)
    normed = plain_part * row_scale * kv_gain.astype(jnp.float32)
    return jnp.concatenate([normed, rotate(latent[:, KVR:], position)], axis=1).astype(jnp.bfloat16)


def turned_dot(a, b):
    return lax.dot_general(a, b, (((0,), (0,)), ((), ())), preferred_element_type=jnp.float32)


def whole_kernel(
    h_ref, ids_ref, gain_ref, router_ref, pages_ref, kv_ref,
    sg_ref, su_ref, sd_ref, eg_ref, eu_ref, ed_ref,
    out_ref, lat_ref,
    x0, xf, xd, sf, sd, p0, pf, pd, q10, q20, q1f, q2f, red, tf, td, acc, xn, hs, gs, rk, wk, pk, lt, lr,
    wg, wu, wd,
    w_sem, a_send, a_recv, g1_send, g1_recv, g2_send, g2_recv, q1_send, q1_recv, q2_send, q2_recv,
    t_send, t_recv, d_send, d_recv, b_send, b_recv, k_send, k_recv, l_send, l_recv,
):
    e = lax.axis_index("ep")
    y = lax.axis_index("tp")
    mx, mz, mc = e // (NZ * NCORE), (e // NCORE) % NZ, e % NCORE
    me = mx * NCORE + mc
    up, down, across = (y + 1) % TP, (y + TP - 1) % TP, (y + 2) % TP
    slots, cap, width = h_ref.shape
    tokens = slots * cap
    f32, bf16 = jnp.float32, jnp.bfloat16

    barrier = pltpu.get_barrier_semaphore()

    def greet(dest):
        pl.semaphore_signal(barrier, inc=1, device_id=dest, device_id_type=pl.DeviceIdType.MESH)

    for k in range(1, TP):
        greet((e, (y + k) % TP))

    def greet_expert(n, carry):
        greet(((e + n) % (NX * NZ * NCORE), y))
        return carry

    lax.fori_loop(1, NX * NZ * NCORE, greet_expert, 0)

    def remote(src, dst, send, recv, dest):
        return pltpu.make_async_remote_copy(
            src_ref=src,
            dst_ref=dst,
            send_sem=send,
            recv_sem=recv,
            device_id=dest,
            device_id_type=pl.DeviceIdType.MESH,
        )

    def ring(src, dst, send, recv, to):
        return remote(src, dst, send, recv, (e, to))

    def gather_one(c, side):
        own = xf.at[c - 1, y]
        return ring(own, own, g1_send.at[c, side], g1_recv.at[c, side], (up, down)[side])

    def gather_two(c, side):
        piece = xf.at[c - 1, (down, up)[side], pl.ds(side * (PLANE // 2), PLANE // 2)]
        return ring(piece, piece, g2_send.at[c, side], g2_recv.at[c, side], (up, down)[side])

    def reduce_one(c, side):
        piece = pf.at[c - 1, across, pl.ds(side * (PLANE // 2), PLANE // 2)]
        return ring(piece, q1f.at[c - 1, side], q1_send.at[c, side], q1_recv.at[c, side], (up, down)[side])

    def reduce_two(c, side):
        piece = pf.at[c - 1, (up, down)[side]]
        return ring(piece, q2f.at[c - 1, side], q2_send.at[c, side], q2_recv.at[c, side], (up, down)[side])

    def shared_gather_one(side):
        return ring(h_ref, x0.at[y], g1_send.at[0, side], g1_recv.at[0, side], (up, down)[side])

    def shared_gather_two(side):
        piece = x0.at[(down, up)[side], pl.ds(side * (slots // 2), slots // 2)]
        return ring(piece, piece, g2_send.at[0, side], g2_recv.at[0, side], (up, down)[side])

    def shared_reduce_one(side):
        piece = p0.at[across, pl.ds(side * (slots // 2), slots // 2)]
        return ring(piece, q10.at[side], q1_send.at[0, side], q1_recv.at[0, side], (up, down)[side])

    def shared_reduce_two(side):
        piece = p0.at[(up, down)[side]]
        return ring(piece, q20.at[side], q2_send.at[0, side], q2_recv.at[0, side], (up, down)[side])

    def picks(k):
        return ring(pk.at[y], pk.at[y], k_send.at[k], k_recv.at[k], (y + k + 1) % TP)

    def latents(k):
        to = (y + k + 1) % TP
        return ring(lt.at[to], lr.at[k], l_send.at[k], l_recv.at[k], to)

    def device(dz, i):
        return ((i // NCORE) * NZ + (mz + dz) % NZ) * NCORE + i % NCORE

    loads = [
        pltpu.make_async_copy(src, dst.at[i], w_sem.at[n])
        for n, (src, dst, i) in enumerate(
            ((sg_ref, wg, 0), (su_ref, wu, 0), (sd_ref, wd, 0), (eg_ref, wg, 1), (eu_ref, wu, 1), (ed_ref, wd, 1))
        )
    ]
    for load in loads:
        load.start()
    x0[y] = h_ref[...]

    groups = rk.shape[0]
    ids = ids_ref[...]
    top = ids.shape[0]
    expert_row = lax.broadcasted_iota(jnp.int32, (groups, tokens), 0)
    chosen = jnp.zeros((groups, tokens), f32)
    for k in range(top):
        chosen = jnp.where(ids[k : k + 1, :] == expert_row, 1.0, chosen)
    earlier = lax.broadcasted_iota(jnp.int32, (tokens, tokens), 0)
    later = lax.broadcasted_iota(jnp.int32, (tokens, tokens), 1)
    before = dot(chosen.astype(bf16), jnp.where(earlier < later, 1.0, 0.0).astype(bf16))
    rk[...] = jnp.where(chosen > 0.0, before, -1.0)
    place = lax.broadcasted_iota(jnp.int32, (cap, tokens), 0).astype(f32)

    def one_hot(s, expert):
        gs[pl.ds(s * cap, cap), :] = jnp.where(rk[pl.ds(expert, 1), :] == place, 1.0, 0.0).astype(bf16)

    def weighted(s, expert):
        gs[pl.ds(s * cap, cap), :] = jnp.where(
            rk[pl.ds(expert, 1), :] == place, wk[pl.ds(expert, 1), :], 0.0
        ).astype(bf16)

    def all_peers(send, skip_self=False):
        def body(n, carry):
            send((me + n) % PLANE)
            return carry

        lax.fori_loop(1 if skip_self else 0, PLANE, body, 0)

    for q, dz in enumerate(FAR):
        for i in range(PLANE):
            one_hot(i, device(dz, i))
        sf[q] = (
            dot(gs[0 : PLANE * cap, :], h_ref[...].reshape(tokens, width))
            .astype(bf16)
            .reshape(PLANE, cap, width)
        )

    pl.semaphore_wait(barrier, NX * NZ * NCORE - 1 + TP - 1)
    for side in range(2):
        shared_gather_one(side).start()

    def far_rows(dz):
        q = FAR.index(dz)

        def straight(i):
            remote(sf.at[q, i], xf.at[q, y, me], a_send, a_recv.at[q], (device(dz, i), y)).start()

        all_peers(straight)

    def norm(count, piece):
        def body(i, carry):
            parts = [piece(i, j).astype(f32) for j in range(TP)]
            energy = sum(jnp.sum(v * v, axis=1, keepdims=True) for v in parts)
            inverse = lax.rsqrt(energy / (width * TP) + EPS)
            at = pl.ds(pl.multiple_of(i * cap, cap), cap)
            for j in range(TP):
                xn[at, j * width : (j + 1) * width] = (
                    parts[j] * inverse * gain_ref[:, j * width : (j + 1) * width]
                ).astype(bf16)
            return carry

        lax.fori_loop(0, count, body, 0)

    def units(rows, w):
        a = xn[0:rows, :]
        hs[0:rows, :] = (silu(dot(a, wg[w])) * dot(a, wu[w])).astype(bf16)

    def down_part(rows, w, j):
        return dot(hs[0:rows, :], wd[w, :, j * width : (j + 1) * width])

    def near_rows(dz):
        k = NEAR.index(dz)
        for i in range(PLANE):
            one_hot(i, device(dz, i))
        for j in range(TP):
            part = dot(gs[0 : PLANE * cap, :], x0[j].reshape(tokens, width)).astype(bf16)
            sd[k * PLANE : (k + 1) * PLANE, j] = part.reshape(PLANE, cap, width)

        def send(i):
            remote(
                sd.at[k * PLANE + i], xd.at[k * PLANE + me], d_send, d_recv.at[k], (device(dz, i), y)
            ).start()

        if dz == 0:
            xd[k * PLANE + me] = sd[k * PLANE + me]
        all_peers(send, dz == 0)

    def shared_part():
        norm(slots, lambda i, j: x0[j, i])
        at = pl.ds(pl.multiple_of(y * width, 128), width)
        logits = dot(xn[0:tokens, at], router_ref[...]).T
        expert = lax.broadcasted_iota(jnp.int32, logits.shape, 0)
        for k in range(top):
            pk[y, k : k + 1, :] = jnp.sum(
                jnp.where(expert == ids_ref[k : k + 1, :], logits, 0.0), axis=0, keepdims=True
            )
        for k in range(TP - 1):
            picks(k).start()
        units(tokens, 0)
        for j in range(TP):
            acc[j] = down_part(tokens, 0, j)

    def near_expert(dz):
        k = NEAR.index(dz)
        most = xd.at[pl.ds(k * PLANE, PLANE - 1 if dz == 0 else PLANE)]
        remote(most, most, d_send, d_recv.at[k], (e, up)).wait_recv()
        norm(PLANE, lambda i, j: xd[k * PLANE + i, j])
        units(PLANE * cap, 1)
        for j in range(TP):
            pd[k * PLANE : (k + 1) * PLANE, j] = (
                down_part(PLANE * cap, 1, j).astype(bf16).reshape(PLANE, cap, width)
            )

        def send_back(i):
            remote(
                pd.at[k * PLANE + i], td.at[k * PLANE + me], b_send, b_recv.at[k], (device(NZ - dz, i), y)
            ).start()

        if dz == 0:
            td[k * PLANE + me] = pd[k * PLANE + me]
        all_peers(send_back, dz == 0)

    def gather_start(c):
        remote(xf.at[c - 1, y], xf.at[c - 1, y], a_send, a_recv.at[c - 1], (e, up)).wait_recv()
        for side in range(2):
            gather_one(c, side).start()

    def gather_on(c):
        for side in range(2):
            gather_one(c, side).wait_recv()
            gather_two(c, side).start()

    def far_expert(c):
        for side in range(2):
            gather_two(c, side).wait_recv()
        norm(PLANE, lambda i, j: xf[c - 1, j, i])
        units(PLANE * cap, 1)
        for j in range(TP):
            pf[c - 1, j] = down_part(PLANE * cap, 1, j).astype(bf16).reshape(PLANE, cap, width)
        for side in range(2):
            reduce_one(c, side).start()

    def reduce_on(c):
        for side in range(2):
            reduce_one(c, side).wait_recv()
            at = pl.ds(side * (PLANE // 2), PLANE // 2)
            to = (up, down)[side]
            pf[c - 1, to, at] = (pf[c - 1, to, at].astype(f32) + q1f[c - 1, side].astype(f32)).astype(bf16)
            reduce_two(c, side).start()

    def far_back(c):
        q, dz = c - 1, FAR[c - 1]
        for side in range(2):
            reduce_two(c, side).wait_recv()
        red[q] = (pf[q, y].astype(f32) + q2f[q, 0].astype(f32) + q2f[q, 1].astype(f32)).astype(bf16)

        def straight(i):
            remote(red.at[q, i], tf.at[q * PLANE + me], t_send, t_recv, (device(NZ - dz, i), y)).start()

        all_peers(straight)

    def shared_on():
        for load in loads:
            load.wait()
        for side in range(2):
            shared_gather_one(side).wait_recv()
            shared_gather_two(side).start()

    def shared_ready():
        for side in range(2):
            shared_gather_two(side).wait_recv()

    def join_near():
        for k in range(TP - 1):
            picks(k).wait()
        scores = 1.0 / (1.0 + jnp.exp(-(pk[0] + pk[1] + pk[2] + pk[3])))
        gates = ROUTE_SCALE * scores / jnp.sum(scores, axis=0, keepdims=True)
        weights = jnp.zeros((groups, tokens), f32)
        for k in range(top):
            weights = jnp.where(ids_ref[k : k + 1, :] == expert_row, gates[k : k + 1, :], weights)
        wk[...] = weights
        for k, dz in enumerate(NEAR):
            for i in range(PLANE):
                weighted(k * PLANE + i, device(dz, i))
            most = td.at[pl.ds(k * PLANE, PLANE - 1 if dz == 0 else PLANE)]
            remote(most, most, b_send, b_recv.at[k], (e, up)).wait_recv()
        for j in range(TP):
            part = acc[j] + turned_dot(gs[0 : NNEAR * cap, :], td[:, j].reshape(NNEAR * cap, width))
            p0[j] = part.astype(bf16).reshape(slots, cap, width)
        for side in range(2):
            shared_reduce_one(side).start()

    def shared_reduce_on():
        for side in range(2):
            shared_reduce_one(side).wait_recv()
            at = pl.ds(side * (slots // 2), slots // 2)
            to = (up, down)[side]
            p0[to, at] = (p0[to, at].astype(f32) + q10[side].astype(f32)).astype(bf16)
            shared_reduce_two(side).start()

    def join_far():
        remote(tf, tf, t_send, t_recv, (e, up)).wait_recv()
        total = h_ref[...].reshape(tokens, width).astype(f32)
        for part in range(2):
            for s in range(HALF):
                slot = part * HALF + s
                weighted(s, device(FAR[slot // PLANE], slot % PLANE))
            total = total + turned_dot(
                gs[0 : HALF * cap, :], tf[part * HALF : (part + 1) * HALF].reshape(HALF * cap, width)
            )
        acc[0] = total

    steps = {
        "a": far_rows,
        "n": near_rows,
        "x": near_expert,
        "s0": lambda dz: gather_start(FAR.index(dz) + 1),
        "s1": lambda dz: gather_on(FAR.index(dz) + 1),
        "s2": lambda dz: far_expert(FAR.index(dz) + 1),
        "s3": lambda dz: reduce_on(FAR.index(dz) + 1),
        "s4": lambda dz: far_back(FAR.index(dz) + 1),
        "sg2": shared_on,
        "sg3": shared_ready,
        "shared": shared_part,
        "f1": join_near,
        "f2": shared_reduce_on,
        "t": join_far,
    }
    for name, *offset in ORDER:
        steps[name](*offset)
    for side in range(2):
        shared_reduce_two(side).wait_recv()
    total = acc[0].reshape(slots, cap, width) + p0[y].astype(f32) + q20[0].astype(f32) + q20[1].astype(f32)
    layer = total.reshape(tokens, width).astype(bf16)
    out_ref[...] = layer

    page = tokens // TP
    token = lax.broadcasted_iota(jnp.int32, (page, tokens), 1)
    inside = lax.broadcasted_iota(jnp.int32, (page, tokens), 0)
    paged = jnp.concatenate(
        [
            dot(jnp.where(token == pages_ref[0, j] * page + inside, 1.0, 0.0).astype(bf16), layer)
            for j in range(TP)
        ],
        axis=0,
    )
    energy = jnp.sum(paged * paged, axis=1, keepdims=True)
    scaled = (paged * gain_ref[:, TP * width :]).astype(bf16)
    latent = lax.dot_general(
        scaled, kv_ref[...], (((1,), (1,)), ((), ())), preferred_element_type=f32
    )
    columns = latent.shape[1]
    spare = (lt.shape[2] - columns) // 2
    coarse = energy.astype(bf16)
    fine = (energy - coarse.astype(f32)).astype(bf16)
    for j in range(TP):
        at = slice(j * page, (j + 1) * page)
        lt[j, :, 0:columns] = latent[at, :].astype(bf16)
        lt[j, :, columns : columns + spare] = jnp.broadcast_to(coarse[at, :], (page, spare))
        lt[j, :, columns + spare :] = jnp.broadcast_to(fine[at, :], (page, spare))
    for k in range(TP - 1):
        latents(k).start()
    for k in range(TP - 1):
        latents(k).wait()
    lat_ref[...] = lt[y].astype(f32) + lr[0].astype(f32) + lr[1].astype(f32) + lr[2].astype(f32)

    for side in range(2):
        shared_gather_one(side).wait_send()
        shared_gather_two(side).wait_send()
        shared_reduce_one(side).wait_send()
        shared_reduce_two(side).wait_send()

    def drain(c, carry):
        for side in range(2):
            gather_one(c, side).wait_send()
            gather_two(c, side).wait_send()
            reduce_one(c, side).wait_send()
            reduce_two(c, side).wait_send()
        return carry

    lax.fori_loop(1, NFAR + 1, drain, 0)
    remote(sf, sf, a_send, t_recv, (e, up)).wait_send()
    remote(red, red, t_send, t_recv, (e, up)).wait_send()
    most = sd.at[pl.ds(0, NNEAR - 1)]
    remote(most, most, d_send, t_recv, (e, up)).wait_send()
    remote(most, most, b_send, t_recv, (e, up)).wait_send()


def whole(hidden, ids, gain, router, pages, kv, weights):
    slots, cap, width = hidden.shape
    tokens = slots * cap
    f32, bf16 = jnp.float32, jnp.bfloat16
    hidden_units = weights[0].shape[1]
    latent = -(-(kv.shape[0] + 1) // 128) * 128
    vmem, hbm = pl.BlockSpec(memory_space=pltpu.VMEM), pl.BlockSpec(memory_space=pl.ANY)
    dma = pltpu.SemaphoreType.DMA
    pair = dma((NFAR + 1, 2))
    block = (slots, cap, width)
    strip = (PLANE, cap, width)
    return pl.pallas_call(
        whole_kernel,
        out_shape=(
            jax.ShapeDtypeStruct((tokens, width), bf16),
            jax.ShapeDtypeStruct((tokens // TP, latent), f32),
        ),
        in_specs=[vmem] * 4 + [pl.BlockSpec(memory_space=pltpu.SMEM), vmem] + [hbm] * 6,
        out_specs=(vmem, vmem),
        scratch_shapes=[
            pltpu.VMEM((TP, *block), bf16),
            pltpu.VMEM((NFAR, TP, *strip), bf16),
            pltpu.VMEM((NNEAR, TP, cap, width), bf16),
            pltpu.VMEM((NFAR, *strip), bf16),
            pltpu.VMEM((NNEAR, TP, cap, width), bf16),
            pltpu.VMEM((TP, *block), bf16),
            pltpu.VMEM((NFAR, TP, *strip), bf16),
            pltpu.VMEM((NNEAR, TP, cap, width), bf16),
            pltpu.VMEM((2, slots // 2, cap, width), bf16),
            pltpu.VMEM((2, *block), bf16),
            pltpu.VMEM((NFAR, 2, PLANE // 2, cap, width), bf16),
            pltpu.VMEM((NFAR, 2, *strip), bf16),
            pltpu.VMEM((NFAR, *strip), bf16),
            pltpu.VMEM((NFAR * PLANE, cap, width), bf16),
            pltpu.VMEM((NNEAR, TP, cap, width), bf16),
            pltpu.VMEM((TP, tokens, width), f32),
            pltpu.VMEM((tokens, width * TP), bf16),
            pltpu.VMEM((tokens, hidden_units), bf16),
            pltpu.VMEM((max(NNEAR, HALF) * cap, tokens), bf16),
            pltpu.VMEM((NX * NZ * NCORE, tokens), f32),
            pltpu.VMEM((NX * NZ * NCORE, tokens), f32),
            pltpu.VMEM((TP, *ids.shape), f32),
            pltpu.VMEM((TP, tokens // TP, latent), bf16),
            pltpu.VMEM((TP - 1, tokens // TP, latent), bf16),
            pltpu.VMEM((2, width * TP, hidden_units), bf16),
            pltpu.VMEM((2, width * TP, hidden_units), bf16),
            pltpu.VMEM((2, hidden_units, width * TP), bf16),
            dma((6,)),
            dma,
            dma((NFAR,)),
            pair, pair, pair, pair, pair, pair, pair, pair,
            dma, dma, dma, dma((len(NEAR),)), dma, dma((len(NEAR),)),
            dma((TP - 1,)), dma((TP - 1,)), dma((TP - 1,)), dma((TP - 1,)),
        ],
        compiler_params=pltpu.CompilerParams(
            collective_id=0, has_side_effects=True, vmem_limit_bytes=67000000
        ),
    )(hidden, ids, gain, router, pages, kv, *weights)


def per_device(
    hidden_in,
    moe_gain,
    router_weight,
    expert_ids,
    shared_gate,
    shared_up,
    shared_down,
    expert_gate,
    expert_up,
    expert_down,
    attn_gain,
    kv_down,
    kv_gain,
    doc_lengths,
    page_table,
):
    tp_count = lax.axis_size("tp")
    member = lax.axis_index("tp")
    tok_rows, width_local = hidden_in.shape
    full_width = width_local * tp_count
    f32 = jnp.float32
    page_count = page_table.shape[1]
    page_len = tok_rows // page_count

    layer_out, sums = whole(
        hidden_in.reshape(tok_rows // CAP, CAP, width_local),
        expert_ids.T,
        jnp.concatenate([moe_gain, attn_gain]).astype(f32).reshape(1, full_width + width_local),
        router_weight,
        page_table,
        kv_down.T,
        (shared_gate, shared_up, shared_down, expert_gate[0], expert_up[0], expert_down[0]),
    )

    slot = jnp.arange(page_count, dtype=jnp.int32)
    own_page = jnp.sum(jnp.where(slot == member, page_table[0], 0))
    tokens = own_page * page_len + jnp.arange(page_len, dtype=jnp.int32)
    columns = kv_down.shape[1]
    latent = sums[:, :columns] * lax.rsqrt(sums[:, columns : columns + 1] / full_width + EPS)
    page_out = finish(latent, positions_of(doc_lengths[0], tokens), kv_gain)
    return (layer_out, page_out.reshape(1, page_count // tp_count, page_len, -1))


def solution(mesh):
    placed = (
        P("ep", "tp"),
        P(),
        P("tp", None),
        P("ep", None),
        P(None, "tp"),
        P(None, "tp"),
        P("tp", None),
        P("ep", None, "tp"),
        P("ep", None, "tp"),
        P("ep", "tp", None),
        P("tp"),
        P("tp", None),
        P(),
        P("ep", None),
        P("ep", None),
    )
    return jax.shard_map(
        per_device,
        mesh=mesh,
        in_specs=placed,
        out_specs=(P("ep", "tp"), P("ep", "tp", None, None)),
        check_vma=False,
    )
```
